32 devices in a mesh: dev: 32 (over z, y, x, core).
Axes of the slice: x: 2, y: 2, z: 4, core: 2. Of those that a mesh axis runs over, the one named last changes fastest.
Arguments:
- pixels: bfloat16 [96, 64, 16], P('dev'), may hold values from -6 to 6
- embed_w: bfloat16 [96, 16, 8192], P('dev'), may hold values from -1.5 to 1.5
- var_embed: bfloat16 [96, 8192], P('dev'), may hold values from -3 to 3
- key_w: bfloat16 [8192, 8192], P('dev'), may hold values from -0.0625 to 0.0625
- query: float32 [8192], replicated, may hold values from -500 to 500
- value_t: bfloat16 [8192, 8192], P('dev'), may hold values from -0.0625 to 0.0625
- out_w: bfloat16 [8192, 8192], P('dev'), may hold values from -0.0625 to 0.0625
Outputs:
- mixed: bfloat16 [64, 8192], P('dev')
The draws below stay inside these ranges and needn't reach their ends.
All inputs are finite; a program needn't handle non-finite values.
Results may differ from the reference program's by a relative error of at most 0.012.
The reference program's roundings to bfloat16 on the way (of `embed`, `attn`, `pooled` and `heads`) count: a program that leaves them out, or rounds other values in their place, can miss the bound.
Values may be sent and summed in bfloat16 or wider, within the bound.
No kernel may reach another device: no remote copies, remote signals or barrier semaphores. Data moves between devices by JAX's collectives and lax.ppermute only.
A program may use at most 64 MiB of HBM per device.

```python
import jax
import jax.numpy as jnp
from jax import lax

D = 8192
HEADS = 64
HD = 128
P_SIZE = 16
V = 91
TOK_DEV = 2
VSLOT = 96
TOKENS = 64
N_DEV = 32


def draw_query(key, part):
    first, second = jax.random.split(jax.random.fold_in(key, 17))
    base = jnp.clip(jax.random.normal(first, (HEADS, HD), jnp.float32), -5.0, 5.0)
    scales = jnp.exp(jax.random.uniform(second, (HEADS, 1), jnp.float32, jnp.log(0.5), jnp.log(3.0)))
    return (base * scales).reshape(HEADS * HD)


def steps_of(key, shape, cuts, low, largest):
    gain = 1.0
    for dim, shards_of in cuts:
        heights = jax.random.uniform(jax.random.fold_in(jax.random.fold_in(key, 6), dim), (shards_of,), jnp.float32, low / len(cuts), largest / len(cuts))
        gain = gain * jnp.repeat(jnp.exp(heights), shape[dim] // shards_of).reshape((-1,) + (1,) * (len(shape) - 1 - dim))
    return gain


def bell_draw(own_key, shape, deviation, reach, shards=(), held_as=jnp.bfloat16):
    array = deviation * jax.random.normal(own_key, shape, jnp.float32)
    if shards:
        array = array * steps_of(own_key, shape, shards, -0.22, 0.18)
    return jnp.clip(array, -reach, reach).astype(held_as)


def setup_inputs(seed: int = 0) -> dict:
    key_of = jax.random.split(jax.random.key(seed), 8)
    pixels = bell_draw(key_of[0], (VSLOT, TOKENS, P_SIZE), 1.0, 6.0, ((0, 32),))
    embed_w = bell_draw(key_of[1], (VSLOT, P_SIZE, D), P_SIZE ** -0.5, 1.5, ((0, 32),))
    var_embed = bell_draw(key_of[2], (VSLOT, D), 0.5, 3.0, ((0, 32),))
    key_w = bell_draw(key_of[3], (D, D), D ** -0.5, 0.0625, ((0, 32),))
    query = draw_query(jax.random.fold_in(key_of[7], 71), 0)
    value_t = bell_draw(key_of[5], (D, D), D ** -0.5, 0.0625, ((0, 32),))
    out_w = bell_draw(key_of[6], (D, D), D ** -0.5, 0.0625, ((0, 32),))
    return {"pixels": pixels, "embed_w": embed_w, "var_embed": var_embed, "key_w": key_w, "query": query, "value_t": value_t, "out_w": out_w}


def reference(pixels, embed_w, var_embed, key_w, query, value_t, out_w):
    query_heads = query.reshape(HEADS, HD)
    keyq = jnp.einsum('dhj,hj->dh', key_w.astype(jnp.float32).reshape(D, HEADS, HD), query_heads, precision=lax.Precision.HIGHEST)
    value_full = value_t.astype(jnp.float32).reshape(HEADS, HD, D)
    live_pixels = pixels[:V].reshape(V, N_DEV, TOK_DEV, P_SIZE).transpose(1, 0, 2, 3)
    live_embed_w = embed_w[:V].astype(jnp.float32)
    live_var = var_embed[:V].astype(jnp.float32)

    def one_block(block):
        embed = jnp.einsum('vtp,vpd->vtd', block.astype(jnp.float32), live_embed_w, precision=lax.Precision.HIGHEST)
        embed = (embed + live_var[:, None, :]).astype(jnp.bfloat16)
        logits = jnp.einsum('vtd,dh->vth', embed.astype(jnp.float32), keyq, precision=lax.Precision.HIGHEST) / jnp.sqrt(jnp.float32(HD))
        row_max = lax.optimization_barrier(jnp.max(logits, axis=0, keepdims=True))
        weights = jnp.exp(logits - row_max)
        attn = (weights / lax.optimization_barrier(jnp.sum(weights, axis=0, keepdims=True))).astype(jnp.bfloat16)
        pooled = jnp.einsum('vth,vtd->thd', attn.astype(jnp.float32), embed.astype(jnp.float32), precision=lax.Precision.HIGHEST).astype(jnp.bfloat16)
        heads = jnp.einsum('thd,hcd->thc', pooled.astype(jnp.float32), value_full, precision=lax.Precision.HIGHEST)
        heads = heads.reshape(TOK_DEV, D).astype(jnp.bfloat16)
        return jnp.dot(heads, out_w, preferred_element_type=jnp.float32).astype(jnp.bfloat16)
    mixed = lax.map(one_block, live_pixels)
    return mixed.reshape(TOKENS, D)
```

```python
import jax
import jax.numpy as jnp
from jax import lax
from jax.sharding import PartitionSpec as P

D = 8192
HEADS = 64
HD = 128
V = 91


def body(pixels, embed_w, var_embed, key_w, query, value_t, out_w):
    group_size = lax.axis_size("dev")
    own_embed = jnp.einsum("vtp,vpd->vtd", pixels, embed_w, preferred_element_type=jnp.float32)
    own_embed = (own_embed + var_embed.astype(jnp.float32)[:, None, :]).astype(jnp.bfloat16)
    grouped = lax.all_to_all(own_embed, "dev", split_axis=1, concat_axis=0, tiled=True)
    key_rows = key_w.shape[0]
    keyq_part = jnp.einsum(
        "dhj,hj->dh",
        key_w.astype(jnp.float32).reshape(key_rows, HEADS, HD),
        query.reshape(HEADS, HD),
        precision=lax.Precision.HIGHEST,
    )
    keyq = lax.all_gather(keyq_part, "dev", axis=0, tiled=True)
    logits = jnp.einsum(
        "vtd,dh->vth", grouped.astype(jnp.float32), keyq, precision=lax.Precision.HIGHEST
    ) / jnp.sqrt(jnp.float32(HD))
    slot = lax.broadcasted_iota(jnp.int32, logits.shape, 0)
    logits = jnp.where(slot < V, logits, -1e30)
    row_max = jnp.max(logits, axis=0, keepdims=True)
    weights = jnp.exp(logits - row_max)
    attn = (weights / jnp.sum(weights, axis=0, keepdims=True)).astype(jnp.bfloat16)
    pooled = jnp.einsum("vth,vtd->thd", attn, grouped, preferred_element_type=jnp.float32).astype(
        jnp.bfloat16
    )
    own_tokens = pooled.shape[0]
    if group_size >= HEADS:
        spread = jnp.repeat(pooled, group_size // HEADS, axis=1)[:, :, None, :]
    else:
        spread = pooled.reshape(own_tokens, group_size, HEADS // group_size, D)
    received = lax.all_to_all(spread, "dev", split_axis=1, concat_axis=0, tiled=True)
    all_tokens = received.shape[0]
    head_share = received.shape[2]
    received = received.reshape(all_tokens, head_share, D)
    columns = value_t.shape[0]
    value_heads = jnp.einsum(
        "thd,hcd->thc",
        received,
        value_t.reshape(head_share, columns // head_share, D),
        preferred_element_type=jnp.float32,
    )
    value_heads = value_heads.reshape(all_tokens, columns).astype(jnp.bfloat16)
    summed = lax.psum_scatter(
        jnp.dot(value_heads, out_w, preferred_element_type=jnp.float32),
        "dev",
        scatter_dimension=0,
        tiled=True,
    )
    return summed.astype(jnp.bfloat16)


def split3(x):
    hi = lax.reduce_precision(x, 8, 7)
    rest = x - hi
    mid = lax.reduce_precision(rest, 8, 7)
    low = lax.reduce_precision(rest - mid, 8, 7)
    return [piece.astype(jnp.bfloat16) for piece in (hi, mid, low)]


def halves_body(pixels, embed_w, var_embed, key_w, query, value_t, out_w):
    n_dev = lax.axis_size("dev")
    half = n_dev // 2
    me = lax.axis_index("dev")
    my_half = me // half
    in_half = [[side * half + i for i in range(half)] for side in range(2)]
    across = [(i, (i + half) % n_dev) for i in range(n_dev)]

    def exchange(x):
        return lax.all_to_all(x, "dev", 0, 0, axis_index_groups=in_half, tiled=True)

    own_v, tokens, p_size = pixels.shape
    width = D // half
    slots = own_v * n_dev
    half_heads = HEADS // 2
    dev_heads = HEADS // n_dev

    w_rows = embed_w.reshape(own_v, p_size, half, width).transpose(2, 0, 1, 3)
    w_rows = w_rows.reshape(half, own_v * p_size, width)
    var_rows = var_embed.reshape(own_v, half, width).transpose(1, 0, 2)
    pix_rows = pixels.transpose(0, 2, 1).reshape(1, -1, width)
    pix_rows = jnp.broadcast_to(pix_rows, (half,) + pix_rows.shape[1:])
    packed = jnp.concatenate([w_rows, var_rows, pix_rows], axis=1)
    n_rows = packed.shape[1]
    packed = jnp.pad(packed, ((0, 0), (0, -n_rows % 16), (0, 0)))
    mine = exchange(packed)
    other = lax.ppermute(mine, "dev", across)
    first = my_half == 0
    both = jnp.concatenate(
        [jnp.where(first, mine, other), jnp.where(first, other, mine)], axis=0
    )
    k = own_v * p_size
    w_all = both[:, :k].reshape(slots, p_size, width)
    var_all = both[:, k : k + own_v].reshape(slots, width)
    pix_all = both[:, k + own_v : n_rows].reshape(slots, p_size, tokens)
    embed = jnp.einsum("vpt,vpd->vtd", pix_all, w_all, preferred_element_type=jnp.float32)
    embed = (embed + var_all.astype(jnp.float32)[:, None, :]).astype(jnp.bfloat16)

    key_rows = key_w.shape[0]
    keyq_part = jnp.einsum(
        "dhj,hj->hd",
        key_w.astype(jnp.float32).reshape(key_rows, HEADS, HD),
        query.reshape(HEADS, HD),
        precision=lax.Precision.HIGHEST,
    )
    odd = me % 2
    low_heads, high_heads = keyq_part[:half_heads], keyq_part[half_heads:]
    to_same = [(i, i // 2 + half * (i % 2)) for i in range(n_dev)]
    to_other = [(i, i // 2 + half * (1 - i % 2)) for i in range(n_dev)]
    got_same = lax.ppermute(jnp.where(odd == 0, low_heads, high_heads), "dev", to_same)
    got_other = lax.ppermute(jnp.where(odd == 0, high_heads, low_heads), "dev", to_other)
    keyq = jnp.concatenate(
        [jnp.where(first, got_same, got_other), jnp.where(first, got_other, got_same)], axis=1
    )
    pieces = jnp.concatenate(split3(keyq), axis=0)
    part = lax.dot_general(
        pieces,
        embed.reshape(slots * tokens, width),
        (((1,), (1,)), ((), ())),
        preferred_element_type=jnp.float32,
    )
    part = part.reshape(3, half_heads, slots * tokens).sum(axis=0)
    part = part.reshape(half, dev_heads * slots * tokens // 128, 128)
    logits = exchange(part).reshape(half, dev_heads, slots, tokens).sum(axis=0)
    logits = logits / jnp.sqrt(jnp.float32(HD))
    slot = lax.broadcasted_iota(jnp.int32, logits.shape, 1)
    logits = jnp.where(slot < V, logits, -1e30)
    row_max = jnp.max(logits, axis=1, keepdims=True)
    weights = jnp.exp(logits - row_max)
    attn = (weights / jnp.sum(weights, axis=1, keepdims=True)).astype(jnp.bfloat16)
    attn = attn.reshape(1, -1, 128)
    attn = exchange(jnp.broadcast_to(attn, (half,) + attn.shape[1:]))
    attn = attn.reshape(half_heads, slots, tokens)

    pooled = jnp.einsum("hvt,vtd->thd", attn, embed, preferred_element_type=jnp.float32).astype(
        jnp.bfloat16
    )
    spread = pooled.reshape(tokens, half, dev_heads, width).transpose(1, 2, 0, 3)
    received = exchange(spread.reshape(half, dev_heads * tokens, width))
    received = received.reshape(half, dev_heads, tokens, width)
    columns = value_t.shape[0]
    value_heads = jnp.einsum(
        "rhtk,hcrk->thc",
        received,
        value_t.reshape(dev_heads, columns // dev_heads, half, width),
        preferred_element_type=jnp.float32,
    )
    value_heads = value_heads.reshape(tokens, columns).astype(jnp.bfloat16)
    sums = jnp.dot(value_heads, out_w, preferred_element_type=jnp.float32).astype(jnp.bfloat16)
    sums = lax.all_to_all(
        sums.reshape(n_dev, -1, 1024), "dev", 0, 0, tiled=True
    )
    summed = jnp.sum(sums.astype(jnp.float32), axis=0)
    return summed.reshape(tokens // n_dev, D).astype(jnp.bfloat16)


def solution(mesh):
    placed = (
        P("dev", None, None),
        P("dev", None, None),
        P("dev", None),
        P("dev", None),
        P(),
        P("dev", None),
        P("dev", None),
    )
    n_dev = mesh.shape["dev"]
    chosen = halves_body if n_dev % 2 == 0 and HEADS % n_dev == 0 else body
    return jax.shard_map(
        chosen, mesh=mesh, in_specs=placed, out_specs=P("dev", None), check_vma=False
    )
```

```python
import jax
import jax.numpy as jnp
from jax import lax
from jax.sharding import PartitionSpec as P


D = 8192
HEADS = 64
HD = 128
V = 91


def body(pixels, embed_w, var_embed, key_w, query, value_t, out_w):
    group_size = lax.axis_size("dev")
    own_embed = jnp.einsum("vtp,vpd->vtd", pixels, embed_w, preferred_element_type=jnp.float32)
    own_embed = (own_embed + var_embed.astype(jnp.float32)[:, None, :]).astype(jnp.bfloat16)
    grouped = lax.all_to_all(own_embed, "dev", split_axis=1, concat_axis=0, tiled=True)
    key_rows = key_w.shape[0]
    keyq_part = jnp.einsum(
        "dhj,hj->dh",
        key_w.astype(jnp.float32).reshape(key_rows, HEADS, HD),
        query.reshape(HEADS, HD),
        precision=lax.Precision.HIGHEST,
    )
    keyq = lax.all_gather(keyq_part, "dev", axis=0, tiled=True)
    logits = jnp.einsum(
        "vtd,dh->vth", grouped.astype(jnp.float32), keyq, precision=lax.Precision.HIGHEST
    ) / jnp.sqrt(jnp.float32(HD))
    slot = lax.broadcasted_iota(jnp.int32, logits.shape, 0)
    logits = jnp.where(slot < V, logits, -1e30)
    row_max = jnp.max(logits, axis=0, keepdims=True)
    weights = jnp.exp(logits - row_max)
    attn = (weights / jnp.sum(weights, axis=0, keepdims=True)).astype(jnp.bfloat16)
    pooled = jnp.einsum("vth,vtd->thd", attn, grouped, preferred_element_type=jnp.float32).astype(
        jnp.bfloat16
    )
    own_tokens = pooled.shape[0]
    if group_size >= HEADS:
        spread = jnp.repeat(pooled, group_size // HEADS, axis=1)[:, :, None, :]
    else:
        spread = pooled.reshape(own_tokens, group_size, HEADS // group_size, D)
    received = lax.all_to_all(spread, "dev", split_axis=1, concat_axis=0, tiled=True)
    all_tokens = received.shape[0]
    head_share = received.shape[2]
    received = received.reshape(all_tokens, head_share, D)
    columns = value_t.shape[0]
    value_heads = jnp.einsum(
        "thd,hcd->thc",
        received,
        value_t.reshape(head_share, columns // head_share, D),
        preferred_element_type=jnp.float32,
    )
    value_heads = value_heads.reshape(all_tokens, columns).astype(jnp.bfloat16)
    summed = lax.psum_scatter(
        jnp.dot(value_heads, out_w, preferred_element_type=jnp.float32),
        "dev",
        scatter_dimension=0,
        tiled=True,
    )
    return summed.astype(jnp.bfloat16)


def split3(x):
    hi = lax.reduce_precision(x, 8, 7)
    rest = x - hi
    mid = lax.reduce_precision(rest, 8, 7)
    low = lax.reduce_precision(rest - mid, 8, 7)
    return [piece.astype(jnp.bfloat16) for piece in (hi, mid, low)]


def halves_body(*args):
    return halves_plan(*args)


def halves_plan(pixels, embed_w, var_embed, key_w, query, value_t, out_w):
    n_dev = lax.axis_size("dev")
    half = n_dev // 2
    me = lax.axis_index("dev")
    my_half = me // half
    in_half = [[side * half + i for i in range(half)] for side in range(2)]
    across = [(i, (i + half) % n_dev) for i in range(n_dev)]

    def exchange(x):
        return lax.all_to_all(x, "dev", 0, 0, axis_index_groups=in_half, tiled=True)

    own_v, tokens, p_size = pixels.shape
    width = D // half
    slots = own_v * n_dev
    half_heads = HEADS // 2
    dev_heads = HEADS // n_dev

    first = my_half == 0
    cut = p_size // 2

    def by_slice(x):
        x = x.reshape(x.shape[0], -1, half, width).transpose(2, 0, 1, 3)
        return x.reshape(half, -1, width)

    def in_order(mine, other):
        return [jnp.where(first, mine, other), jnp.where(first, other, mine)]

    pix_lanes = pixels.transpose(0, 2, 1).reshape(own_v, p_size * tokens)
    small = jnp.concatenate([var_embed, pix_lanes], axis=1)
    small_other = lax.ppermute(small, "dev", across)
    early = embed_w[:, :cut]
    early_other = lax.ppermute(early, "dev", across)
    small_both = jnp.concatenate(in_order(small, small_other), axis=0)
    var_rows = by_slice(small_both[:, :D])
    pix_rows = small_both[:, D:].reshape(1, -1, width)
    pix_rows = jnp.broadcast_to(pix_rows, (half,) + pix_rows.shape[1:])
    packed = jnp.concatenate([by_slice(embed_w[:, cut:]), var_rows, pix_rows], axis=1)
    n_rows = packed.shape[1]
    packed = jnp.pad(packed, ((0, 0), (0, -n_rows % 16), (0, 0)))
    packed = exchange(packed)
    k = own_v * (p_size - cut)
    late = packed[:, :k]
    late_other = lax.ppermute(late, "dev", across)
    early_other, late = lax.optimization_barrier((early_other, late))
    small_v = packed[:, k : k + 2 * own_v].reshape(half, 2, own_v, width)
    var_all = small_v.transpose(1, 0, 2, 3).reshape(slots, width)
    pix_all = packed[:, k + 2 * own_v : n_rows].reshape(half, 2, own_v, p_size, tokens)
    pix_all = pix_all.transpose(1, 0, 2, 3, 4).reshape(slots, p_size, tokens)
    early = by_slice(jnp.concatenate(in_order(early, early_other), axis=0))
    early = exchange(early)
    early = early.reshape(half, 2, own_v, cut, width).transpose(1, 0, 2, 3, 4)
    late = jnp.stack(in_order(late, late_other)).reshape(2, half, own_v, -1, width)
    w_all = jnp.concatenate([early, late], axis=3).reshape(slots, p_size, width)
    embed = jnp.einsum("vpt,vpd->vtd", pix_all, w_all, preferred_element_type=jnp.float32)
    embed = (embed + var_all.astype(jnp.float32)[:, None, :]).astype(jnp.bfloat16)

    key_rows = key_w.shape[0]
    keyq_part = jnp.einsum(
        "dhj,hj->hd",
        key_w.astype(jnp.float32).reshape(key_rows, HEADS, HD),
        query.reshape(HEADS, HD),
        precision=lax.Precision.HIGHEST,
    )
    odd = me % 2
    low_heads, high_heads = keyq_part[:half_heads], keyq_part[half_heads:]
    to_same = [(i, i // 2 + half * (i % 2)) for i in range(n_dev)]
    to_other = [(i, i // 2 + half * (1 - i % 2)) for i in range(n_dev)]
    got_same = lax.ppermute(jnp.where(odd == 0, low_heads, high_heads), "dev", to_same)
    got_other = lax.ppermute(jnp.where(odd == 0, high_heads, low_heads), "dev", to_other)
    keyq = jnp.concatenate(
        [jnp.where(first, got_same, got_other), jnp.where(first, got_other, got_same)], axis=1
    )
    pieces = jnp.concatenate(split3(keyq), axis=0)
    part = lax.dot_general(
        pieces,
        embed.reshape(slots * tokens, width),
        (((1,), (1,)), ((), ())),
        preferred_element_type=jnp.float32,
    )
    part = part.reshape(3, half_heads, slots * tokens).sum(axis=0)
    part = part.reshape(half, dev_heads * slots * tokens // 128, 128)
    logits = exchange(part).reshape(half, dev_heads, slots, tokens).sum(axis=0)
    logits = logits / jnp.sqrt(jnp.float32(HD))
    slot = lax.broadcasted_iota(jnp.int32, logits.shape, 1)
    logits = jnp.where(slot < V, logits, -1e30)
    row_max = jnp.max(logits, axis=1, keepdims=True)
    weights = jnp.exp(logits - row_max)
    attn = (weights / jnp.sum(weights, axis=1, keepdims=True)).astype(jnp.bfloat16)
    attn = attn.reshape(1, -1, 128)
    attn = exchange(jnp.broadcast_to(attn, (half,) + attn.shape[1:]))
    attn = attn.reshape(half_heads, slots, tokens)

    pooled = jnp.einsum("hvt,vtd->thd", attn, embed, preferred_element_type=jnp.float32).astype(
        jnp.bfloat16
    )
    spread = pooled.reshape(tokens, half, dev_heads, width).transpose(1, 2, 0, 3)
    received = exchange(spread.reshape(half, dev_heads * tokens, width))
    received = received.reshape(half, dev_heads, tokens, width)
    columns = value_t.shape[0]
    value_heads = jnp.einsum(
        "rhtk,hcrk->thc",
        received,
        value_t.reshape(dev_heads, columns // dev_heads, half, width),
        preferred_element_type=jnp.float32,
    )
    value_heads = value_heads.reshape(tokens, columns).astype(jnp.bfloat16)
    side = me % 2
    rows = value_heads.reshape(half, 2, -1, columns).transpose(1, 0, 2, 3)
    rows = rows.reshape(2, tokens // 2, columns)

    def sums_for(who):
        picked = lax.dynamic_index_in_dim(rows, who, 0, keepdims=False)
        return jnp.dot(picked, out_w, preferred_element_type=jnp.float32)

    swap = [(i, i ^ 1) for i in range(n_dev)]
    sums = lax.ppermute(sums_for(1 - side), "dev", swap) + sums_for(side)
    same_side = [[2 * i + c for i in range(half)] for c in range(2)]
    sums = lax.all_to_all(
        sums.astype(jnp.bfloat16).reshape(half, -1, 1024),
        "dev", 0, 0, axis_index_groups=same_side, tiled=True,
    )
    summed = jnp.sum(sums.astype(jnp.float32), axis=0)
    return summed.reshape(tokens // n_dev, D).astype(jnp.bfloat16)


def solution(mesh):
    placed = (
        P("dev", None, None),
        P("dev", None, None),
        P("dev", None),
        P("dev", None),
        P(),
        P("dev", None),
        P("dev", None),
    )
    n_dev = mesh.shape["dev"]
    halves = n_dev % 2 == 0 and HEADS % n_dev == 0
    chosen = halves_body if halves else body
    return jax.shard_map(
        chosen, mesh=mesh, in_specs=placed, out_specs=P("dev", None), check_vma=False
    )
```
